32 devices in a mesh: row: 4 (over y, x), col: 8 (over z, core).
Axes of the slice: x: 2, y: 2, z: 4, core: 2. Of those that a mesh axis runs over, the one named last changes fastest.
Arguments:
- tiles: bfloat16 [4, 8, 128, 128, 128], P('row', 'col'), may hold values from 0 to 0.31
- block_rows: int32 [4, 8, 128], P('row', 'col'), may hold values from 0 to 63, as said below
- block_cols: int32 [4, 8, 128], P('row', 'col'), may hold values from 0 to 127
- counts: int32 [4, 8], P('row', 'col'), may hold values from 1 to 128, as said below
- seeds: int32 [8, 65536], P(None, ('col', 'row')), may hold values from 1 to 999
Outputs:
- vectors_out: float32 [8, 65536], P(None, ('col', 'row'))
- deltas: float32 [4, 8], replicated
The draws below stay inside these ranges and needn't reach their ends.
Inputs may be any that keep to these rules, and one draw needn't show every extreme that they name: `counts`: each entry is 1, a half, a quarter or an eighth of 128 (at least 1); some device is full in every draw. On each device, among the values of block_rows (over all 128 slots) that share one quotient by 16, at most 4 are distinct; on a device whose count is 128, some quotient has exactly 4 distinct values among its tiles.
All inputs are finite; a program needn't handle non-finite values.
Results may differ from the reference program's by a relative error of at most 0.00061.
Values may be sent and summed in bfloat16 or wider, within the bound.
A program may use at most 64 MiB of HBM per device.

```python
import jax
import jax.numpy as jnp
from jax import lax

K = 8
BLOCK = 128
ITERS = 4
PIECE_DEV = 2048
TILES_DEV = 128
NODES = 65536
ROW_BLOCKS = 64
COL_BLOCKS = 128
ROW_CAP = 4
N_ROW = 4
N_COL = 8


def draw_counts(key, part):
    level_key = jax.random.fold_in(key, 11)
    spot_key = jax.random.fold_in(key, 23)
    levels = jax.random.randint(level_key, (N_ROW * N_COL,), 0, 4)
    divided = TILES_DEV // jnp.power(2, levels).astype(jnp.int32)
    divided = jnp.maximum(divided, 1).astype(jnp.int32)
    chosen = jax.random.randint(spot_key, (), 0, N_ROW * N_COL)
    divided = divided.at[chosen].set(TILES_DEV)
    return divided.reshape(N_ROW, N_COL).astype(jnp.int32)


def distinct_order(key, rows, length):
    scores = jax.random.randint(key, (rows, length), 0, 1 << 20) * length + jnp.arange(length, dtype=jnp.int32)[None, :]
    return jnp.argsort(scores, axis=1).astype(jnp.int32)


def draw_block_rows(key, part):
    piece_blocks = PIECE_DEV // BLOCK
    devices_all = N_ROW * N_COL
    allowed_total = N_ROW * ROW_CAP
    offsets = distinct_order(jax.random.fold_in(key, 31), devices_all * N_ROW, piece_blocks)[:, :ROW_CAP]
    offsets = offsets.reshape(devices_all, N_ROW, ROW_CAP)
    owners = jnp.arange(N_ROW, dtype=jnp.int32)[None, :, None] * piece_blocks
    allowed = (owners + offsets).reshape(devices_all, allowed_total).astype(jnp.int32)
    ranks = distinct_order(jax.random.fold_in(key, 37), devices_all, TILES_DEV)
    picks = jax.random.randint(jax.random.fold_in(key, 41), (devices_all, TILES_DEV), 0, allowed_total)
    index = jnp.where(ranks < allowed_total, ranks, picks).astype(jnp.int32)
    chosen = jnp.take_along_axis(allowed, index, axis=1)
    return chosen.reshape(N_ROW, N_COL, TILES_DEV).astype(jnp.int32)


def row_classes(key):
    return jax.random.randint(jax.random.fold_in(key, 53), (NODES // BLOCK,), 0, 2).astype(jnp.int32)


def draw_tiles(key, part):
    mask_key = jax.random.fold_in(key, 5)
    weight_key = jax.random.fold_in(key, 7)
    shape = (N_ROW, N_COL, TILES_DEV, BLOCK, BLOCK)
    density = min(0.5, 16.0 * PIECE_DEV / (BLOCK * BLOCK * TILES_DEV))
    kept = jax.random.uniform(mask_key, shape, dtype=jnp.float32) < density
    local_rows = draw_block_rows(key, part)
    segment_base = jnp.arange(N_COL, dtype=jnp.int32)[None, :, None] * ROW_BLOCKS
    classes = row_classes(key)[(local_rows + segment_base).astype(jnp.int32)]
    heavy_rows = (classes == 1)[:, :, :, None, None]
    spread = jax.random.uniform(weight_key, shape, dtype=jnp.float32)
    light_weight = jnp.exp(jnp.log(0.01) + spread * (jnp.log(0.04) - jnp.log(0.01)))
    heavy_weight = jnp.exp(jnp.log(0.12) + spread * (jnp.log(0.3) - jnp.log(0.12)))
    weights = jnp.where(heavy_rows, heavy_weight, light_weight)
    return jnp.where(kept, weights, 0.0).astype(jnp.bfloat16)


def draw_seeds(key, part):
    node_index = jnp.arange(NODES, dtype=jnp.int32)
    node_block = (node_index // BLOCK).astype(jnp.int32)
    node_class = row_classes(key)[node_block]
    threshold = jax.random.randint(jax.random.fold_in(key, 61), (K, 1), 4, 9)
    rolls = jax.random.randint(jax.random.fold_in(key, 67), (K, NODES // BLOCK), 0, 8)
    node_rolls = rolls[:, node_block]
    raised = jnp.where(node_class[None, :] == 0, node_rolls < threshold, node_rolls < 1)
    high_value = jax.random.randint(jax.random.fold_in(key, 71), (K, NODES), 500, 1000)
    low_value = jax.random.randint(jax.random.fold_in(key, 73), (K, NODES), 1, 40)
    return jnp.where(raised, high_value, low_value).astype(jnp.int32)


def set_ends(result, key, least, top_value):
    longest = result.shape.index(max(result.shape))
    spots = []
    for shift in (0, 1):
        where = [jax.random.randint(jax.random.fold_in(key, axis), (), 0, length) for axis, length in enumerate(result.shape)]
        where[longest] = (where[longest] + shift) % result.shape[longest]
        spots.append(tuple(where))
    return result.at[spots[0]].set(least).at[spots[1]].set(top_value)


def setup_inputs(seed: int = 0) -> dict:
    arg_keys = jax.random.split(jax.random.key(seed), 6)
    tiles = draw_tiles(jax.random.fold_in(arg_keys[5], 71), 0)
    block_rows = draw_block_rows(jax.random.fold_in(arg_keys[5], 71), 0)
    block_cols = set_ends(jax.random.randint(arg_keys[2], (N_ROW, N_COL, TILES_DEV), 0, COL_BLOCKS), jax.random.fold_in(arg_keys[2], 1), 0, COL_BLOCKS - 1).astype(jnp.int32)
    counts = draw_counts(jax.random.fold_in(arg_keys[5], 71), 0)
    seeds = draw_seeds(jax.random.fold_in(arg_keys[5], 71), 0)
    return {"tiles": tiles, "block_rows": block_rows, "block_cols": block_cols, "counts": counts, "seeds": seeds}


def reference(tiles, block_rows, block_cols, counts, seeds):
    piece_blocks = PIECE_DEV // BLOCK
    row_span = N_ROW * piece_blocks
    total_nodes = PIECE_DEV * N_ROW * N_COL
    devices_all = N_ROW * N_COL
    all_blocks = total_nodes // BLOCK
    flat_tiles = tiles.reshape(devices_all, TILES_DEV, BLOCK, BLOCK)
    flat_rows = block_rows.reshape(devices_all, TILES_DEV).astype(jnp.int32)
    flat_cols = block_cols.reshape(devices_all, TILES_DEV).astype(jnp.int32)
    flat_counts = counts.reshape(devices_all).astype(jnp.int32)
    positions = jnp.arange(devices_all, dtype=jnp.int32)
    row_index = positions // N_COL
    col_index = positions % N_COL
    tile_index = jnp.arange(TILES_DEV, dtype=jnp.int32)
    global_rows = (col_index[:, None] * row_span + flat_rows).astype(jnp.int32)
    global_cols = (((flat_cols // piece_blocks) * N_ROW + row_index[:, None]) * piece_blocks + flat_cols % piece_blocks).astype(jnp.int32)
    live_mask = (tile_index[None, :] < flat_counts[:, None]).astype(jnp.float32)

    def add_degree(running, entry_data):
        panel_here, rows_here, live_here = entry_data
        row_total = jnp.sum(panel_here.astype(jnp.float32), axis=2) * live_here[:, None]
        return running.at[rows_here].add(row_total), None

    degree = lax.scan(add_degree, jnp.zeros((all_blocks, BLOCK), jnp.float32), (flat_tiles, global_rows, live_mask))[0]
    divisor = 1.0 + degree[:, None, :]
    seed_float = seeds.astype(jnp.float32)
    start_vec = total_nodes * seed_float / jnp.sum(seed_float, axis=1, keepdims=True)
    current = start_vec.reshape(K, all_blocks, BLOCK).transpose(1, 0, 2)
    deltas = []
    for iteration in range(ITERS):
        half_vec = lax.optimization_barrier(current.astype(jnp.bfloat16))

        def add_product(running, entry_data, source=half_vec):
            panel_here, rows_here, cols_here, live_here = entry_data
            taken_rows = source[cols_here].astype(jnp.float32)
            product = jnp.einsum("tkc,trc->tkr", taken_rows, panel_here.astype(jnp.float32), precision=lax.Precision.HIGHEST)
            return running.at[rows_here].add(product * live_here[:, None, None]), None

        image = lax.scan(add_product, jnp.zeros((all_blocks, K, BLOCK), jnp.float32), (flat_tiles, global_rows, global_cols, live_mask))[0]
        raw_next = (image + current) / divisor
        totals = jnp.sum(raw_next, axis=(0, 2))
        updated = total_nodes * raw_next / totals[None, :, None]
        deltas.append(jnp.max(jnp.abs(updated - current), axis=(0, 2)))
        current = updated
    return current.transpose(1, 0, 2).reshape(K, total_nodes), jnp.stack(deltas)
```

```python
import functools

import jax
import jax.numpy as jnp
from jax import lax
from jax.experimental import pallas as pl
from jax.experimental.pallas import tpu as pltpu
from jax.sharding import PartitionSpec as P

BLOCK = 128
ITERS = 4
ROW_CAP = 4
CHUNK = 16
STEP = 4
MESH = pl.DeviceIdType.MESH


def kernel(
    n_row,
    n_col,
    total_nodes,
    targets,
    cols,
    slot_ids,
    tiles,
    seeds,
    out,
    deltas_out,
    panel,
    gath,
    table,
    hist,
    inv_deg,
    part,
    landed,
    deg_send,
    deg_recv,
    tot_send,
    tot_recv,
    tile_sem,
    gs_sem,
    gr_sem,
    rs_sem,
    rr_sem,
    ds_sem,
    dr_sem,
    ts_sem,
    tr_sem,
):
    vectors = seeds.shape[0]
    piece_blocks = seeds.shape[1] // BLOCK
    devices = n_row * n_col
    chips = n_col // 2
    slots = n_row * ROW_CAP
    chunks = panel.shape[0]
    row = lax.axis_index("row")
    col = lax.axis_index("col")
    me = row * n_col + col
    z = col // 2
    core = col % 2
    partner = z * 2 + (1 - core)

    def tile_copy(chunk, t):
        return pltpu.make_async_copy(
            tiles.at[0, 0, chunk * CHUNK + t],
            panel.at[chunk, :, pl.ds(t * BLOCK, BLOCK)],
            tile_sem.at[chunk],
        )

    def start_tiles(chunk, carry):
        for t in range(CHUNK):
            tile_copy(chunk, t).start()
        return carry

    lax.fori_loop(0, chunks, start_tiles, 0)

    barrier = pltpu.get_barrier_semaphore()

    def greet(d, carry):
        f = lax.rem(me + d, devices)
        pl.semaphore_signal(
            barrier, inc=1, device_id=(f // n_col, f % n_col), device_id_type=MESH
        )
        return carry

    lax.fori_loop(1, devices, greet, 0)

    lane = lax.broadcasted_iota(jnp.int32, (vectors, BLOCK), 1)
    sub = lax.broadcasted_iota(jnp.int32, (vectors, BLOCK), 0)

    def to_row(value, base=0):
        return jnp.sum(jnp.where(lane == sub + base, value, 0.0), axis=0, keepdims=True)

    def to_column(value):
        return jnp.sum(jnp.where(lane == sub, value, 0.0), axis=1, keepdims=True)

    def exchange_copy(which, d):
        f = lax.rem(me + d, devices)
        return pltpu.make_async_remote_copy(
            src_ref=tot_send.at[which],
            dst_ref=tot_recv.at[which, d],
            send_sem=ts_sem.at[which],
            recv_sem=tr_sem.at[which],
            device_id=(f // n_col, f % n_col),
            device_id_type=MESH,
        )

    def share(which, value):
        tot_send[which] = value
        tot_recv[which, 0] = value

        def go(d, carry):
            exchange_copy(which, d).start()
            return carry

        lax.fori_loop(1, devices, go, 0)

    def shared(which):
        rest = tot_recv.at[which, pl.ds(1, devices - 1)]
        pltpu.make_async_copy(rest, rest, tr_sem.at[which]).wait()
        return tot_recv[which]

    seed_sum = jnp.zeros((vectors, BLOCK), jnp.float32)
    for b in range(piece_blocks):
        value = seeds[:, b * BLOCK : (b + 1) * BLOCK].astype(jnp.float32)
        hist[0, b] = value
        seed_sum = seed_sum + value
    pl.semaphore_wait(barrier, devices - 1)
    share(0, to_row(jnp.sum(seed_sum, axis=1, keepdims=True)))

    slot_row = lax.broadcasted_iota(jnp.int32, (slots, BLOCK), 0)

    def degree_chunk(chunk, acc):
        pltpu.make_async_copy(panel.at[chunk], panel.at[chunk], tile_sem.at[chunk]).wait()
        pieces = []
        for t in range(CHUNK):
            hit = slot_row == targets[chunk * CHUNK + t]
            pieces.append(jnp.where(hit, 1.0, 0.0).astype(jnp.bfloat16))
        return acc + lax.dot_general(
            jnp.concatenate(pieces, axis=1),
            panel[chunk],
            (((1,), (1,)), ((), ())),
            preferred_element_type=jnp.float32,
        )

    degree = lax.fori_loop(0, chunks, degree_chunk, jnp.zeros((slots, BLOCK), jnp.float32))
    for o in range(n_row):
        ids = [
            jnp.full((1, BLOCK), slot_ids[o * ROW_CAP + s], jnp.int32).astype(jnp.float32)
            for s in range(ROW_CAP)
        ]
        deg_send[o] = jnp.concatenate([degree[o * ROW_CAP : (o + 1) * ROW_CAP]] + ids, axis=0)

    def degree_copy(d):
        to = lax.rem(row + d, n_row)
        return pltpu.make_async_remote_copy(
            src_ref=deg_send.at[to],
            dst_ref=deg_recv.at[row],
            send_sem=ds_sem.at[d],
            recv_sem=dr_sem.at[d],
            device_id=(to, col),
            device_id_type=MESH,
        )

    for d in range(1, n_row):
        degree_copy(d).start()
    deg_recv[row] = deg_send[row]

    def own_copy(it):
        own = gath.at[it, pl.ds(col * piece_blocks, piece_blocks)]
        return pltpu.make_async_remote_copy(
            src_ref=hist.at[it],
            dst_ref=own,
            send_sem=gs_sem.at[it, 0],
            recv_sem=gr_sem.at[it, 0],
            device_id=(row, partner),
            device_id_type=MESH,
        )

    def far_copy(it, d):
        to = lax.rem(z + d, chips) * 2 + core
        own = gath.at[it, pl.ds(col * piece_blocks, piece_blocks)]
        return pltpu.make_async_remote_copy(
            src_ref=hist.at[it],
            dst_ref=own,
            send_sem=gs_sem.at[it, d],
            recv_sem=gr_sem.at[it, d],
            device_id=(row, to),
            device_id_type=MESH,
        )

    def pass_copy(it, d):
        source = lax.rem(z - d + chips, chips) * 2 + core
        there = gath.at[it, pl.ds(source * piece_blocks, piece_blocks)]
        return pltpu.make_async_remote_copy(
            src_ref=there,
            dst_ref=there,
            send_sem=gs_sem.at[it, chips - 1 + d],
            recv_sem=gr_sem.at[it, chips - 1 + d],
            device_id=(row, partner),
            device_id_type=MESH,
        )

    def part_copy(it, d):
        to = lax.rem(row + d, n_row)
        return pltpu.make_async_remote_copy(
            src_ref=part.at[it, to],
            dst_ref=landed.at[it, row],
            send_sem=rs_sem.at[it, d],
            recv_sem=rr_sem.at[it, d],
            device_id=(to, col),
            device_id_type=MESH,
        )

    slot_of_row = (
        lax.broadcasted_iota(jnp.int32, (slots * vectors, BLOCK), 0) // vectors
    ).astype(jnp.float32).astype(jnp.bfloat16)

    def fill_table(it, scale, b):
        value = gath[it, b] * scale
        table[b] = jnp.concatenate([value, value], axis=0).astype(jnp.bfloat16)

    def product_chunk(chunk, acc):
        for g in range(CHUNK // STEP):
            pieces = []
            for s in range(STEP):
                t = g * STEP + s
                at = chunk * CHUNK + t
                taken = table[cols[at]]
                wide = jnp.concatenate([taken] * (slots * vectors // (2 * vectors)), axis=0)
                mine = jnp.full((slots * vectors, BLOCK), targets[at], jnp.int32)
                mine = mine.astype(jnp.float32).astype(jnp.bfloat16)
                pieces.append(jnp.where(slot_of_row == mine, wide, jnp.zeros_like(wide)))
            acc = acc + lax.dot_general(
                jnp.concatenate(pieces, axis=1),
                panel[chunk, :, g * STEP * BLOCK : (g + 1) * STEP * BLOCK],
                (((1,), (1,)), ((), ())),
                preferred_element_type=jnp.float32,
            )
        return acc

    def own_delta(it, scale, scale_before):
        worst = jnp.zeros((vectors, BLOCK), jnp.float32)
        for b in range(piece_blocks):
            change = hist[it + 1, b] * scale - hist[it, b] * scale_before
            worst = jnp.maximum(worst, jnp.abs(change))
        return to_row(jnp.max(worst, axis=1, keepdims=True), it * vectors)

    delta_row = jnp.zeros((1, BLOCK), jnp.float32)
    scale_before = None
    for it in range(ITERS):
        for d in range(1, chips):
            far_copy(it, d).start()
        own_copy(it).start()
        gath[it, pl.ds(col * piece_blocks, piece_blocks)] = hist[it]
        scale = total_nodes / to_column(jnp.sum(shared(it), axis=0))
        if it > 0:
            delta_row = delta_row + own_delta(it - 1, scale, scale_before)
        scale_before = scale
        for d in range(1, chips):
            far_copy(it, d).wait_recv()
            pass_copy(it, d).start()
        own_copy(it).wait_recv()
        for d in range(1, chips):
            pass_copy(it, d).wait_recv()

        @pl.loop(0, gath.shape[1], unroll=8)
        def _(b, it=it, scale=scale):
            fill_table(it, scale, b)

        acc = lax.fori_loop(
            0, chunks, product_chunk, jnp.zeros((slots * vectors, BLOCK), jnp.float32)
        )
        part[it] = acc.reshape(n_row, ROW_CAP * vectors, BLOCK)
        for d in range(1, n_row):
            part_copy(it, d).start()
        landed[it, row] = part[it, row]
        if it == 0:
            for d in range(1, n_row):
                degree_copy(d).wait_recv()
            for p in range(piece_blocks):
                found = jnp.ones((1, BLOCK), jnp.float32)
                for j in range(n_row):
                    for s in range(ROW_CAP):
                        where_to = deg_recv[j, ROW_CAP + s : ROW_CAP + s + 1]
                        found = found + jnp.where(
                            where_to == float(p), deg_recv[j, s : s + 1], 0.0
                        )
                inv_deg[p] = jnp.broadcast_to(1.0 / found, (vectors, BLOCK))
        for d in range(1, n_row):
            part_copy(it, d).wait_recv()
        sums = [hist[it, p] * scale for p in range(piece_blocks)]
        for j in range(n_row):
            for s in range(ROW_CAP):
                value = landed[it, j, s * vectors : (s + 1) * vectors]
                where_to = jnp.broadcast_to(
                    deg_recv[j, ROW_CAP + s : ROW_CAP + s + 1], (vectors, BLOCK)
                )
                for p in range(piece_blocks):
                    sums[p] = sums[p] + jnp.where(where_to == float(p), value, 0.0)
        local = jnp.zeros((vectors, BLOCK), jnp.float32)
        for p in range(piece_blocks):
            fresh = sums[p] * inv_deg[p]
            hist[it + 1, p] = fresh
            local = local + fresh
        share(it + 1, to_row(jnp.sum(local, axis=1, keepdims=True)))

    scale = total_nodes / to_column(jnp.sum(shared(ITERS), axis=0))
    delta_row = delta_row + own_delta(ITERS - 1, scale, scale_before)
    share(ITERS + 1, delta_row)
    for b in range(piece_blocks):
        out[:, b * BLOCK : (b + 1) * BLOCK] = hist[ITERS, b] * scale
    for d in range(1, n_row):
        degree_copy(d).wait_send()
    for it in range(ITERS):
        own_copy(it).wait_send()
        for d in range(1, chips):
            far_copy(it, d).wait_send()
            pass_copy(it, d).wait_send()
        for d in range(1, n_row):
            part_copy(it, d).wait_send()
    top = jnp.max(shared(ITERS + 1), axis=0)
    for n in range(ITERS):
        deltas_out[n : n + 1, :] = top[:, n * vectors : (n + 1) * vectors]
    for which in range(ITERS + 2):
        rest = tot_recv.at[which, pl.ds(1, devices - 1)]
        pltpu.make_async_copy(rest, rest, ts_sem.at[which]).wait()


def on_device(tiles, block_rows, block_cols, counts, seeds):
    n_row = lax.axis_size("row")
    n_col = lax.axis_size("col")
    vectors = seeds.shape[0]
    piece_blocks = seeds.shape[1] // BLOCK
    tile_total = tiles.shape[2]
    slots = n_row * ROW_CAP
    span = n_row * piece_blocks
    chunks = tile_total // CHUNK
    devices = n_row * n_col
    rows = block_rows[0, 0]
    live = jnp.arange(tile_total, dtype=jnp.int32) < counts[0, 0]
    blocks = jnp.arange(span, dtype=jnp.int32)
    hits = (rows[None, :] == blocks[:, None]) & live[None, :]
    present = jnp.max(hits.astype(jnp.int32), axis=1)
    earlier = (blocks[None, :] < blocks[:, None]) & (
        blocks[None, :] // piece_blocks == blocks[:, None] // piece_blocks
    )
    rank = jnp.sum(jnp.where(earlier, present[None, :], 0), axis=1)
    slot = (blocks // piece_blocks) * ROW_CAP + rank
    targets = jnp.sum(jnp.where(hits, slot[:, None] + 1, 0), axis=0) - 1
    slot_index = jnp.arange(slots, dtype=jnp.int32)
    match = (slot[:, None] == slot_index[None, :]) & (present[:, None] == 1)
    slot_ids = jnp.sum(jnp.where(match, (blocks % piece_blocks)[:, None], 0), axis=0)

    smem = pl.BlockSpec(memory_space=pltpu.SMEM)
    vmem = pl.BlockSpec(memory_space=pltpu.VMEM)
    f32, bf16 = jnp.float32, jnp.bfloat16
    dma = pltpu.SemaphoreType.DMA
    out, deltas = pl.pallas_call(
        functools.partial(kernel, n_row, n_col, float(seeds.shape[1] * devices)),
        out_shape=(
            jax.ShapeDtypeStruct(seeds.shape, f32),
            jax.ShapeDtypeStruct((ITERS, vectors), f32),
        ),
        in_specs=[smem, smem, smem, pl.BlockSpec(memory_space=pl.ANY), vmem],
        out_specs=(vmem, vmem),
        scratch_shapes=[
            pltpu.VMEM((chunks, BLOCK, CHUNK * BLOCK), bf16),
            pltpu.VMEM((ITERS, n_col * piece_blocks, vectors, BLOCK), f32),
            pltpu.VMEM((n_col * piece_blocks, 2 * vectors, BLOCK), bf16),
            pltpu.VMEM((ITERS + 1, piece_blocks, vectors, BLOCK), f32),
            pltpu.VMEM((piece_blocks, vectors, BLOCK), f32),
            pltpu.VMEM((ITERS, n_row, ROW_CAP * vectors, BLOCK), f32),
            pltpu.VMEM((ITERS, n_row, ROW_CAP * vectors, BLOCK), f32),
            pltpu.VMEM((n_row, 2 * ROW_CAP, BLOCK), f32),
            pltpu.VMEM((n_row, 2 * ROW_CAP, BLOCK), f32),
            pltpu.VMEM((ITERS + 2, 1, BLOCK), f32),
            pltpu.VMEM((ITERS + 2, devices, 1, BLOCK), f32),
            dma((chunks,)),
            dma((ITERS, n_col)),
            dma((ITERS, n_col)),
            dma((ITERS, n_row)),
            dma((ITERS, n_row)),
            dma((n_row,)),
            dma((n_row,)),
            dma((ITERS + 2,)),
            dma((ITERS + 2,)),
        ],
        compiler_params=pltpu.CompilerParams(collective_id=0, has_side_effects=True),
    )(targets, block_cols[0, 0], slot_ids, tiles, seeds)
    return out, deltas


def solution(mesh):
    placed = (
        P("row", "col", None, None, None),
        P("row", "col", None),
        P("row", "col", None),
        P("row", "col"),
        P(None, ("col", "row")),
    )
    return jax.shard_map(
        on_device,
        mesh=mesh,
        in_specs=placed,
        out_specs=(P(None, ("col", "row")), P()),
        check_vma=False,
    )
```

```python
import functools

import jax
import jax.numpy as jnp
from jax import lax
from jax.experimental import pallas as pl
from jax.experimental.pallas import tpu as pltpu
from jax.sharding import PartitionSpec as P

BLOCK = 128
ITERS = 4
ROW_CAP = 4
RAW_ITERS = 2
CHUNK = 16
STEP = 4
MESH = pl.DeviceIdType.MESH


def kernel(
    n_row,
    n_col,
    total_nodes,
    targets,
    cols,
    slot_ids,
    rows,
    live_cols,
    tiles,
    seeds,
    out,
    deltas_out,
    panel,
    gath,
    gath_half,
    half,
    table,
    hist,
    inv_deg,
    part,
    landed,
    deg_send,
    deg_recv,
    tot_send,
    tot_recv,
    inv_send,
    inv_recv,
    inv_split,
    col_parts,
    col_send,
    col_recv,
    tile_sem,
    gs_sem,
    gr_sem,
    rs_sem,
    rr_sem,
    ds_sem,
    dr_sem,
    ts_sem,
    tr_sem,
    is_sem,
    ir_sem,
    ws_sem,
    wr_sem,
):
    vectors = seeds.shape[0]
    piece_blocks = seeds.shape[1] // BLOCK
    devices = n_row * n_col
    chips = n_col // 2
    slots = n_row * ROW_CAP
    chunks = panel.shape[0]
    row = lax.axis_index("row")
    col = lax.axis_index("col")
    me = row * n_col + col
    z = col // 2
    core = col % 2
    partner = z * 2 + (1 - core)

    def tile_copy(chunk, t):
        return pltpu.make_async_copy(
            tiles.at[0, 0, chunk * CHUNK + t],
            panel.at[chunk, :, pl.ds(t * BLOCK, BLOCK)],
            tile_sem.at[chunk],
        )

    def start_tiles(chunk, carry):
        for t in range(CHUNK):
            tile_copy(chunk, t).start()
        return carry

    lax.fori_loop(0, chunks, start_tiles, 0)

    barrier = pltpu.get_barrier_semaphore()

    def greet(d, carry):
        f = lax.rem(me + d, devices)
        pl.semaphore_signal(
            barrier, inc=1, device_id=(f // n_col, f % n_col), device_id_type=MESH
        )
        return carry

    lax.fori_loop(1, devices, greet, 0)

    lane = lax.broadcasted_iota(jnp.int32, (vectors, BLOCK), 1)
    sub = lax.broadcasted_iota(jnp.int32, (vectors, BLOCK), 0)

    def to_row(value, base=0):
        return jnp.sum(jnp.where(lane == sub + base, value, 0.0), axis=0, keepdims=True)

    def to_column(value):
        return jnp.sum(jnp.where(lane == sub, value, 0.0), axis=1, keepdims=True)

    def exchange_copy(which, d):
        f = lax.rem(me + d, devices)
        return pltpu.make_async_remote_copy(
            src_ref=tot_send.at[which],
            dst_ref=tot_recv.at[which, d],
            send_sem=ts_sem.at[which],
            recv_sem=tr_sem.at[which],
            device_id=(f // n_col, f % n_col),
            device_id_type=MESH,
        )

    def share(which, value):
        tot_send[which] = value
        tot_recv[which, 0] = value

        def go(d, carry):
            exchange_copy(which, d).start()
            return carry

        lax.fori_loop(1, devices, go, 0)

    def shared(which):
        rest = tot_recv.at[which, pl.ds(1, devices - 1)]
        pltpu.make_async_copy(rest, rest, tr_sem.at[which]).wait()
        return tot_recv[which]

    seed_sum = jnp.zeros((vectors, BLOCK), jnp.float32)
    for b in range(piece_blocks):
        value = seeds[:, b * BLOCK : (b + 1) * BLOCK].astype(jnp.float32)
        hist[0, b] = value
        seed_sum = seed_sum + value
    pl.semaphore_wait(barrier, devices - 1)
    share(0, to_row(jnp.sum(seed_sum, axis=1, keepdims=True)))

    slot_row = lax.broadcasted_iota(jnp.int32, (slots, BLOCK), 0)

    def degree_chunk(chunk, acc):
        pltpu.make_async_copy(panel.at[chunk], panel.at[chunk], tile_sem.at[chunk]).wait()
        pieces = []
        for t in range(CHUNK):
            hit = slot_row == targets[chunk * CHUNK + t]
            pieces.append(jnp.where(hit, 1.0, 0.0).astype(jnp.bfloat16))
        return acc + lax.dot_general(
            jnp.concatenate(pieces, axis=1),
            panel[chunk],
            (((1,), (1,)), ((), ())),
            preferred_element_type=jnp.float32,
        )

    degree = lax.fori_loop(0, chunks, degree_chunk, jnp.zeros((slots, BLOCK), jnp.float32))
    for o in range(n_row):
        ids = [
            jnp.full((1, BLOCK), slot_ids[o * ROW_CAP + s], jnp.int32).astype(jnp.float32)
            for s in range(ROW_CAP)
        ]
        deg_send[o] = jnp.concatenate([degree[o * ROW_CAP : (o + 1) * ROW_CAP]] + ids, axis=0)

    def degree_copy(d):
        to = lax.rem(row + d, n_row)
        return pltpu.make_async_remote_copy(
            src_ref=deg_send.at[to],
            dst_ref=deg_recv.at[row],
            send_sem=ds_sem.at[d],
            recv_sem=dr_sem.at[d],
            device_id=(to, col),
            device_id_type=MESH,
        )

    for d in range(1, n_row):
        degree_copy(d).start()
    deg_recv[row] = deg_send[row]

    def pieces_of(it, owner):
        held = gath.at[it] if it < RAW_ITERS else gath_half.at[it - RAW_ITERS]
        return held.at[pl.ds(owner * piece_blocks, piece_blocks)]

    def piece_source(it):
        return hist.at[it] if it < RAW_ITERS else half.at[it - RAW_ITERS]

    def own_copy(it):
        own = pieces_of(it, col)
        return pltpu.make_async_remote_copy(
            src_ref=piece_source(it),
            dst_ref=own,
            send_sem=gs_sem.at[it, 0],
            recv_sem=gr_sem.at[it, 0],
            device_id=(row, partner),
            device_id_type=MESH,
        )

    def far_copy(it, d):
        to = lax.rem(z + d, chips) * 2 + core
        own = pieces_of(it, col)
        return pltpu.make_async_remote_copy(
            src_ref=piece_source(it),
            dst_ref=own,
            send_sem=gs_sem.at[it, d],
            recv_sem=gr_sem.at[it, d],
            device_id=(row, to),
            device_id_type=MESH,
        )

    def pass_copy(it, d):
        source = lax.rem(z - d + chips, chips) * 2 + core
        there = pieces_of(it, source)
        return pltpu.make_async_remote_copy(
            src_ref=there,
            dst_ref=there,
            send_sem=gs_sem.at[it, chips - 1 + d],
            recv_sem=gr_sem.at[it, chips - 1 + d],
            device_id=(row, partner),
            device_id_type=MESH,
        )

    def part_copy(it, d):
        to = lax.rem(row + d, n_row)
        return pltpu.make_async_remote_copy(
            src_ref=part.at[it, to],
            dst_ref=landed.at[it, row],
            send_sem=rs_sem.at[it, d],
            recv_sem=rr_sem.at[it, d],
            device_id=(to, col),
            device_id_type=MESH,
        )

    slot_of_row = (
        lax.broadcasted_iota(jnp.int32, (slots * vectors, BLOCK), 0) // vectors
    ).astype(jnp.float32).astype(jnp.bfloat16)

    def fill_table(it, scale, b):
        value = gath[it, b] * scale if it < RAW_ITERS else gath_half[it - RAW_ITERS, b].astype(jnp.float32)
        table[b] = jnp.concatenate([value, value], axis=0).astype(jnp.bfloat16)

    def product_chunk(chunk, acc):
        for g in range(CHUNK // STEP):
            pieces = []
            for s in range(STEP):
                t = g * STEP + s
                at = chunk * CHUNK + t
                taken = table[cols[at]]
                wide = jnp.concatenate([taken] * (slots * vectors // (2 * vectors)), axis=0)
                mine = jnp.full((slots * vectors, BLOCK), targets[at], jnp.int32)
                mine = mine.astype(jnp.float32).astype(jnp.bfloat16)
                pieces.append(jnp.where(slot_of_row == mine, wide, jnp.zeros_like(wide)))
            acc = acc + lax.dot_general(
                jnp.concatenate(pieces, axis=1),
                panel[chunk, :, g * STEP * BLOCK : (g + 1) * STEP * BLOCK],
                (((1,), (1,)), ((), ())),
                preferred_element_type=jnp.float32,
            )
        return acc

    def own_delta(it, scale, scale_before):
        worst = jnp.zeros((vectors, BLOCK), jnp.float32)
        for b in range(piece_blocks):
            change = hist[it + 1, b] * scale - hist[it, b] * scale_before
            worst = jnp.maximum(worst, jnp.abs(change))
        return to_row(jnp.max(worst, axis=1, keepdims=True), it * vectors)

    def inverse_copy(d):
        to = lax.rem(row + d, n_row)
        return pltpu.make_async_remote_copy(
            src_ref=inv_send,
            dst_ref=inv_recv.at[pl.ds(row * piece_blocks, piece_blocks)],
            send_sem=is_sem.at[d],
            recv_sem=ir_sem.at[d],
            device_id=(to, col),
            device_id_type=MESH,
        )

    def column_copy(d):
        to = lax.rem(col + d, n_col)
        return pltpu.make_async_remote_copy(
            src_ref=col_send.at[to],
            dst_ref=col_recv.at[col],
            send_sem=ws_sem.at[d],
            recv_sem=wr_sem.at[d],
            device_id=(row, to),
            device_id_type=MESH,
        )

    def degree_inverse():
        for d in range(1, n_row):
            degree_copy(d).wait_recv()
        for p in range(piece_blocks):
            found = jnp.ones((1, BLOCK), jnp.float32)
            for j in range(n_row):
                for s in range(ROW_CAP):
                    where_to = deg_recv[j, ROW_CAP + s : ROW_CAP + s + 1]
                    found = found + jnp.where(
                        where_to == float(p), deg_recv[j, s : s + 1], 0.0
                    )
            inverse = 1.0 / found
            inv_send[p] = inverse
            inv_deg[p] = jnp.broadcast_to(inverse, (vectors, BLOCK))
        for d in range(1, n_row):
            inverse_copy(d).start()
        inv_recv[pl.ds(row * piece_blocks, piece_blocks)] = inv_send[...]

    def split(value):
        high = value.astype(jnp.bfloat16).astype(jnp.float32)
        rest = value - high
        middle = rest.astype(jnp.bfloat16).astype(jnp.float32)
        return high, middle, rest - middle

    def column_chunk(chunk, carry):
        found = []
        for t in range(CHUNK):
            product = lax.dot_general(
                inv_split[rows[chunk * CHUNK + t]],
                panel[chunk, :, t * BLOCK : (t + 1) * BLOCK],
                (((1,), (0,)), ((), ())),
                preferred_element_type=jnp.float32,
            )
            found.append(jnp.sum(product, axis=0, keepdims=True))
        col_parts[chunk] = jnp.concatenate(found, axis=0)
        return carry

    def column_parts():
        for d in range(1, n_row):
            inverse_copy(d).wait_recv()
        pad = jnp.zeros((2 * vectors - 3, BLOCK), jnp.float32)

        @pl.loop(0, n_row * piece_blocks, unroll=8)
        def _(b):
            inv_split[b] = jnp.concatenate([*split(inv_recv[b]), pad], axis=0).astype(
                jnp.bfloat16
            )

        lax.fori_loop(0, chunks, column_chunk, 0)
        blocks = n_col * piece_blocks
        pick = lax.broadcasted_iota(jnp.int32, (blocks, chunks * CHUNK), 0) == live_cols[...]
        pick = jnp.where(pick, 1.0, 0.0).astype(jnp.bfloat16)
        held = col_parts[...].reshape(chunks * CHUNK, BLOCK)
        gathered = jnp.zeros((blocks, BLOCK), jnp.float32)
        for term in split(held):
            gathered = gathered + jnp.dot(
                pick, term.astype(jnp.bfloat16), preferred_element_type=jnp.float32
            )
        col_send[...] = gathered.reshape(n_col, piece_blocks, BLOCK)
        for d in range(1, n_col):
            column_copy(d).start()
        col_recv[col] = col_send[col]

    def share_ahead(it, scale, column_sum):
        ahead = jnp.zeros((vectors, BLOCK), jnp.float32)
        for b in range(piece_blocks):
            value = hist[it, b] * scale
            rounded = value.astype(jnp.bfloat16).astype(jnp.float32)
            ahead = ahead + column_sum[b : b + 1] * rounded + inv_deg[b] * value
        share(it + 1, to_row(jnp.sum(ahead, axis=1, keepdims=True)))

    delta_row = jnp.zeros((1, BLOCK), jnp.float32)
    column_sum = None
    scale_before = None
    for it in range(ITERS):
        mine = pl.ds(col * piece_blocks, piece_blocks)
        if it >= RAW_ITERS:
            scale = total_nodes / to_column(jnp.sum(shared(it), axis=0))
            for b in range(piece_blocks):
                half[it - RAW_ITERS, b] = (hist[it, b] * scale).astype(jnp.bfloat16)
        for d in range(1, chips):
            far_copy(it, d).start()
        own_copy(it).start()
        if it >= RAW_ITERS:
            gath_half[it - RAW_ITERS, mine] = half[it - RAW_ITERS]
        else:
            gath[it, mine] = hist[it]
        if it == 0:
            degree_inverse()
        if it < RAW_ITERS:
            scale = total_nodes / to_column(jnp.sum(shared(it), axis=0))
        if it == 1:
            for d in range(1, n_col):
                column_copy(d).wait_recv()
            column_sum = jnp.sum(col_recv[...], axis=0)
        if it >= 1:
            share_ahead(it, scale, column_sum)
        if it > 0:
            delta_row = delta_row + own_delta(it - 1, scale, scale_before)
        scale_before = scale
        for d in range(1, chips):
            far_copy(it, d).wait_recv()
            pass_copy(it, d).start()
        own_copy(it).wait_recv()
        for d in range(1, chips):
            pass_copy(it, d).wait_recv()

        @pl.loop(0, gath.shape[1], unroll=8)
        def _(b, it=it, scale=scale):
            fill_table(it, scale, b)

        acc = lax.fori_loop(
            0, chunks, product_chunk, jnp.zeros((slots * vectors, BLOCK), jnp.float32)
        )
        part[it] = acc.reshape(n_row, ROW_CAP * vectors, BLOCK)
        for d in range(1, n_row):
            part_copy(it, d).start()
        landed[it, row] = part[it, row]
        if it == 0:
            column_parts()
        for d in range(1, n_row):
            part_copy(it, d).wait_recv()
        sums = [hist[it, p] * scale for p in range(piece_blocks)]
        for j in range(n_row):
            for s in range(ROW_CAP):
                value = landed[it, j, s * vectors : (s + 1) * vectors]
                where_to = jnp.broadcast_to(
                    deg_recv[j, ROW_CAP + s : ROW_CAP + s + 1], (vectors, BLOCK)
                )
                for p in range(piece_blocks):
                    sums[p] = sums[p] + jnp.where(where_to == float(p), value, 0.0)
        local = jnp.zeros((vectors, BLOCK), jnp.float32)
        for p in range(piece_blocks):
            fresh = sums[p] * inv_deg[p]
            hist[it + 1, p] = fresh
            local = local + fresh
        if it == 0:
            share(1, to_row(jnp.sum(local, axis=1, keepdims=True)))

    scale = total_nodes / to_column(jnp.sum(shared(ITERS), axis=0))
    delta_row = delta_row + own_delta(ITERS - 1, scale, scale_before)
    share(ITERS + 1, delta_row)
    for b in range(piece_blocks):
        out[:, b * BLOCK : (b + 1) * BLOCK] = hist[ITERS, b] * scale
    for d in range(1, n_row):
        degree_copy(d).wait_send()
        inverse_copy(d).wait_send()
    for d in range(1, n_col):
        column_copy(d).wait_send()
    for it in range(ITERS):
        own_copy(it).wait_send()
        for d in range(1, chips):
            far_copy(it, d).wait_send()
            pass_copy(it, d).wait_send()
        for d in range(1, n_row):
            part_copy(it, d).wait_send()
    top = jnp.max(shared(ITERS + 1), axis=0)
    for n in range(ITERS):
        deltas_out[n : n + 1, :] = top[:, n * vectors : (n + 1) * vectors]
    for which in range(ITERS + 2):
        rest = tot_recv.at[which, pl.ds(1, devices - 1)]
        pltpu.make_async_copy(rest, rest, ts_sem.at[which]).wait()


def on_device(tiles, block_rows, block_cols, counts, seeds):
    n_row = lax.axis_size("row")
    n_col = lax.axis_size("col")
    vectors = seeds.shape[0]
    piece_blocks = seeds.shape[1] // BLOCK
    tile_total = tiles.shape[2]
    slots = n_row * ROW_CAP
    span = n_row * piece_blocks
    chunks = tile_total // CHUNK
    devices = n_row * n_col
    rows = block_rows[0, 0]
    live = jnp.arange(tile_total, dtype=jnp.int32) < counts[0, 0]
    blocks = jnp.arange(span, dtype=jnp.int32)
    hits = (rows[None, :] == blocks[:, None]) & live[None, :]
    present = jnp.max(hits.astype(jnp.int32), axis=1)
    earlier = (blocks[None, :] < blocks[:, None]) & (
        blocks[None, :] // piece_blocks == blocks[:, None] // piece_blocks
    )
    rank = jnp.sum(jnp.where(earlier, present[None, :], 0), axis=1)
    slot = (blocks // piece_blocks) * ROW_CAP + rank
    targets = jnp.sum(jnp.where(hits, slot[:, None] + 1, 0), axis=0) - 1
    slot_index = jnp.arange(slots, dtype=jnp.int32)
    match = (slot[:, None] == slot_index[None, :]) & (present[:, None] == 1)
    slot_ids = jnp.sum(jnp.where(match, (blocks % piece_blocks)[:, None], 0), axis=0)

    live_cols = jnp.where(live, block_cols[0, 0], -1)[None, :]
    smem = pl.BlockSpec(memory_space=pltpu.SMEM)
    vmem = pl.BlockSpec(memory_space=pltpu.VMEM)
    f32, bf16 = jnp.float32, jnp.bfloat16
    dma = pltpu.SemaphoreType.DMA
    out, deltas = pl.pallas_call(
        functools.partial(kernel, n_row, n_col, float(seeds.shape[1] * devices)),
        out_shape=(
            jax.ShapeDtypeStruct(seeds.shape, f32),
            jax.ShapeDtypeStruct((ITERS, vectors), f32),
        ),
        in_specs=[smem, smem, smem, smem, vmem, pl.BlockSpec(memory_space=pl.ANY), vmem],
        out_specs=(vmem, vmem),
        scratch_shapes=[
            pltpu.VMEM((chunks, BLOCK, CHUNK * BLOCK), bf16),
            pltpu.VMEM((RAW_ITERS, n_col * piece_blocks, vectors, BLOCK), f32),
            pltpu.VMEM((ITERS - RAW_ITERS, n_col * piece_blocks, vectors, BLOCK), bf16),
            pltpu.VMEM((ITERS - RAW_ITERS, piece_blocks, vectors, BLOCK), bf16),
            pltpu.VMEM((n_col * piece_blocks, 2 * vectors, BLOCK), bf16),
            pltpu.VMEM((ITERS + 1, piece_blocks, vectors, BLOCK), f32),
            pltpu.VMEM((piece_blocks, vectors, BLOCK), f32),
            pltpu.VMEM((ITERS, n_row, ROW_CAP * vectors, BLOCK), f32),
            pltpu.VMEM((ITERS, n_row, ROW_CAP * vectors, BLOCK), f32),
            pltpu.VMEM((n_row, 2 * ROW_CAP, BLOCK), f32),
            pltpu.VMEM((n_row, 2 * ROW_CAP, BLOCK), f32),
            pltpu.VMEM((ITERS + 2, 1, BLOCK), f32),
            pltpu.VMEM((ITERS + 2, devices, 1, BLOCK), f32),
            pltpu.VMEM((piece_blocks, 1, BLOCK), f32),
            pltpu.VMEM((span, 1, BLOCK), f32),
            pltpu.VMEM((span, 2 * vectors, BLOCK), bf16),
            pltpu.VMEM((chunks, CHUNK, BLOCK), f32),
            pltpu.VMEM((n_col, piece_blocks, BLOCK), f32),
            pltpu.VMEM((n_col, piece_blocks, BLOCK), f32),
            dma((chunks,)),
            dma((ITERS, n_col)),
            dma((ITERS, n_col)),
            dma((ITERS, n_row)),
            dma((ITERS, n_row)),
            dma((n_row,)),
            dma((n_row,)),
            dma((ITERS + 2,)),
            dma((ITERS + 2,)),
            dma((n_row,)),
            dma((n_row,)),
            dma((n_col,)),
            dma((n_col,)),
        ],
        compiler_params=pltpu.CompilerParams(collective_id=0, has_side_effects=True),
    )(targets, block_cols[0, 0], slot_ids, rows, live_cols, tiles, seeds)
    return out, deltas


def solution(mesh):
    placed = (
        P("row", "col", None, None, None),
        P("row", "col", None),
        P("row", "col", None),
        P("row", "col"),
        P(None, ("col", "row")),
    )
    return jax.shard_map(
        on_device,
        mesh=mesh,
        in_specs=placed,
        out_specs=(P(None, ("col", "row")), P()),
        check_vma=False,
    )
```
